256 devices in a mesh: tower: 2 (over x_lo), blk: 128 (over z, y, x_hi, core).
Axes of the slice: x: 4 (x_hi: 2, x_lo: 2; x = x_hi * 2 + x_lo), y: 4, z: 8, core: 2. Of those that a mesh axis runs over, the one named last changes fastest.
Arguments:
- pooled: bfloat16 [2, 16384, 1152], P('tower', 'blk'), may hold values from -6 to 6
- final_gain: float32 [2, 1152], P('tower'), may hold values from 0.5 to 1.5
- head_weight: bfloat16 [2, 1152, 1152], P('tower'), may hold values from -0.1875 to 0.1875
- pair_ids: int32 [16384], replicated, may hold values from 0 to 16383
- log_scale: float32 [1], replicated, may hold values from 4.2 to 4.7
- bias: float32 [1], replicated, may hold values from -4 to -1
Outputs:
- emb_grad: float32 [2, 16384, 1152], P('tower', 'blk')
The draws below stay inside these ranges and needn't reach their ends.
Inputs may be any that keep to these rules, and one draw needn't show every extreme that they name: `pair_ids`: examples with equal ids form positive pairs; every example is a positive pair with its own image and text.
All inputs are finite; a program needn't handle non-finite values.
Results may differ from the reference program's by a relative error of at most 0.0043.
Values may be sent and summed in bfloat16 or wider, within the bound.
No kernel may reach another device: no remote copies, remote signals or barrier semaphores. Data moves between devices by JAX's collectives and lax.ppermute only.
A program may use at most 192 MiB of HBM per device.

```python
import jax
import jax.numpy as jnp
from jax import lax

D = 1152
EX_DEV = 128
BATCH = 16384


def set_ends(entries, rng, low, top_value):
    extent = entries.shape
    place = [jax.random.randint(jax.random.fold_in(rng, axis), (), 0, extent[axis]) for axis in range(len(extent))]
    entries = entries.at[tuple(place)].set(low)
    longest = extent.index(max(extent))
    place[longest] = (place[longest] + 1) % extent[longest]
    return entries.at[tuple(place)].set(top_value)


def levels(rng, dims, split, low, high):
    def one(dim, blocks):
        steps = jax.random.uniform(jax.random.fold_in(jax.random.fold_in(rng, 6), dim), (blocks,), jnp.float32, low / len(split), high / len(split))
        return jnp.repeat(jnp.exp(steps), dims[dim] // blocks).reshape((-1,) + (1,) * (len(dims) - dim - 1))

    level = one(*split[0])
    for cut in split[1:]:
        level = level * one(*cut)
    return level


def bell_draw(rng, dims, width, bound, pieces=(), kind=jnp.bfloat16):
    array = width * jax.random.normal(rng, dims, jnp.float32)
    if pieces:
        array = array * levels(rng, dims, pieces, -0.22, 0.18)
    return jnp.clip(array, -bound, bound).astype(kind)


def setup_inputs(seed: int = 0) -> dict:
    key_list = jax.random.split(jax.random.key(seed), 7)
    pooled = bell_draw(key_list[0], (2, BATCH, D), 1.0, 6.0, ((0, 2), (1, 128)))
    final_gain = jnp.clip(0.5 + 1.0 * jax.random.uniform(key_list[1], (2, D), jnp.float32) ** levels(key_list[1], (2, D), ((0, 2),), -0.2, 0.2), 0.5, 1.5)
    head_weight = bell_draw(key_list[2], (2, D, D), D ** -0.5, 0.1875, ((0, 2),))
    pair_ids = set_ends(jax.random.randint(key_list[3], (BATCH,), 0, BATCH), jax.random.fold_in(key_list[3], 1), 0, BATCH - 1).astype(jnp.int32)
    log_scale = jnp.clip(jax.random.uniform(key_list[4], (1,), jnp.float32, 4.2, 4.7), 4.2, 4.7)
    bias = jnp.clip(jax.random.uniform(key_list[5], (1,), jnp.float32, -4.0, -1.0), -4.0, -1.0)
    return {"pooled": pooled, "final_gain": final_gain, "head_weight": head_weight, "pair_ids": pair_ids, "log_scale": log_scale, "bias": bias}


def embed_rows(feats, gain, weight):
    values = feats.astype(jnp.float32)
    center = values - lax.optimization_barrier(jnp.mean(values, axis=-1, keepdims=True))
    spread = lax.optimization_barrier(jnp.mean(center * center, axis=-1, keepdims=True))
    normed = (center * lax.rsqrt(spread + 1e-06) * gain).astype(jnp.bfloat16)
    head = jnp.dot(normed, weight, preferred_element_type=jnp.float32)
    length = lax.optimization_barrier(jnp.sum(head * head, axis=-1, keepdims=True))
    return (head * lax.rsqrt(length + 1e-06)).astype(jnp.bfloat16)

def pair_forces(fixed_rows, moving_rows, fixed_ids, moving_ids, scale, shift):
    logits = scale * lax.dot_general(fixed_rows, moving_rows, (((1,), (1,)), ((), ())), preferred_element_type=jnp.float32) + shift
    sign = jnp.where(fixed_ids[:, None] == moving_ids[None, :], jnp.float32(1.0), jnp.float32(-1.0))
    coef = (-sign * jax.nn.sigmoid(-sign * logits)).astype(jnp.bfloat16)
    return jnp.dot(coef, moving_rows, preferred_element_type=jnp.float32)

def reference(pooled, final_gain, head_weight, pair_ids, log_scale, bias):
    images = embed_rows(pooled[0], final_gain[0], head_weight[0])
    texts = embed_rows(pooled[1], final_gain[1], head_weight[1])
    scale = jnp.exp(log_scale[0])
    shift = bias[0]
    blocks = BATCH // EX_DEV
    id_blocks = pair_ids.reshape(blocks, EX_DEV)

    def image_block(item):
        rows, ids = item
        return pair_forces(rows, texts, ids, pair_ids, scale, shift)

    def text_block(item):
        rows, ids = item
        return pair_forces(rows, images, ids, pair_ids, scale, shift)
    image_grad = lax.map(image_block, (images.reshape(blocks, EX_DEV, D), id_blocks)).reshape(BATCH, D)
    text_grad = lax.map(text_block, (texts.reshape(blocks, EX_DEV, D), id_blocks)).reshape(BATCH, D)
    return jnp.stack([image_grad, text_grad])
```

```python
import jax
import jax.numpy as jnp
from jax import lax
from jax.sharding import PartitionSpec as P

NZ, NY, NH, NC = 8, 4, 2, 2
BLK = NZ * NY * NH * NC


def hop(value, route):
    pairs = []
    for m in range(2):
        for b in range(BLK):
            c, h, y, z = b % NC, b // NC % NH, b // (NC * NH) % NY, b // (NC * NH * NY)
            goal = route(m, z, y, h, c)
            if goal is None:
                continue
            tm, tz, ty, th, tc = goal
            target = ((tz % NZ * NY + ty % NY) * NH + th) * NC + tc
            pairs.append((m * BLK + b, tm * BLK + target))
    return lax.ppermute(value, ("tower", "blk"), pairs)


def embed_rows(feats, gain, weight):
    values = feats.astype(jnp.float32)
    center = values - jnp.mean(values, axis=-1, keepdims=True)
    spread = jnp.mean(center * center, axis=-1, keepdims=True)
    normed = (center * lax.rsqrt(spread + 1e-06) * gain).astype(jnp.bfloat16)
    head = jnp.dot(normed, weight, preferred_element_type=jnp.float32)
    length = jnp.sum(head * head, axis=-1, keepdims=True)
    return (head * lax.rsqrt(length + 1e-06)).astype(jnp.bfloat16)


def pair_coef(image_rows, text_rows, image_ids, text_ids, scale, shift):
    logits = (
        scale
        * lax.dot_general(
            image_rows, text_rows, (((1,), (1,)), ((), ())), preferred_element_type=jnp.float32
        )
        + shift
    )
    match = image_ids[:, None] == text_ids[None, :]
    share = jax.nn.sigmoid(jnp.where(match, -logits, logits))
    return jnp.where(match, -share, share).astype(jnp.bfloat16)


def on_device(pooled, final_gain, head_weight, pair_ids, log_scale, bias):
    bf16, f32 = jnp.bfloat16, jnp.float32
    local = embed_rows(pooled[0], final_gain[0], head_weight[0])
    ex = local.shape[0]
    half = ex // 2
    scale = jnp.exp(log_scale[0])
    shift = bias[0]
    m = lax.axis_index("tower")
    b = lax.axis_index("blk")
    c, h, y, z = b % NC, b // NC % NH, b // (NC * NH) % NY, b // (NC * NH * NY)
    first = c == 0
    image_side = m == 0

    p1 = hop(local, lambda m, z, y, h, c: (0, z, y, h, c) if m else ((1, z, y, h, 1) if c else None))
    p2 = hop(local, lambda m, z, y, h, c: (0, z, y, 1 - h, c) if m else ((1, z, y, h, 0) if c else None))
    p3 = hop(local, lambda m, z, y, h, c: (1, z, y, 1 - h, c) if m else (None if c else (0, z, y, h, 1)))
    text_own = jnp.where(image_side, p1, local)
    text_oth = jnp.where(image_side, p2, p3)
    image = jnp.where(image_side, jnp.where(first, local, p3), jnp.where(first, p2, p1))

    up_y = lambda m, z, y, h, c: (m, z, y + 1, h, c)
    down_y = lambda m, z, y, h, c: (m, z, y - 1, h, c)
    below = [hop(text_own, up_y), hop(text_oth, up_y)]
    above = [hop(text_own, down_y), hop(text_oth, down_y)]
    far = [hop(below[0], up_y), hop(above[1], down_y)]
    texts = [text_own, text_oth] + below + above + far

    ring = lambda m, z, y, h, c: (m, z - 1 if c else z + 1, y, h, c)
    unring = lambda m, z, y, h, c: (m, z + 1 if c else z - 1, y, h, c)
    swap = lambda m, z, y, h, c: (m, z, y, h, 1 - c)
    got, images = image, [image]
    for _ in range(NZ // 2 - 1):
        got = hop(got, ring)
        images += [got, hop(got, swap)]
    last = hop(jnp.where(first, got[:half], got[half:]), ring)
    last_oth = hop(last, swap)
    images.append(
        jnp.where(first, jnp.concatenate([last, last_oth]), jnp.concatenate([last_oth, last]))
    )

    ids = pair_ids.reshape(NZ, NY, NH, NC, ex)
    image_col = lax.dynamic_slice(ids, (0, y, h, m, 0), (NZ, 1, 1, 1, ex)).reshape(NZ, ex)
    step = jnp.where(first, -1, 1)
    image_order = [0] + [s for k in range(1, NZ // 2) for s in (k, -k)] + [NZ // 2]
    image_ids = jnp.concatenate(
        [lax.dynamic_slice_in_dim(image_col, (z + step * k) % NZ, 1)[0] for k in image_order]
    )
    text_col = lax.dynamic_slice(ids, (z, 0, 0, c, 0), (1, NY, NH, 1, ex)).reshape(NY * NH, ex)
    text_order = [(0, 0), (0, 1), (-1, 0), (-1, 1), (1, 0), (1, 1), (2, 0), (2, 1)]
    text_ids = jnp.concatenate(
        [
            lax.dynamic_slice_in_dim(text_col, (y + dy) % NY * NH + (h if dh == 0 else 1 - h), 1)[0]
            for dy, dh in text_order
        ]
    )

    image_rows = jnp.concatenate(images)
    text_rows = jnp.concatenate(texts)
    coef = pair_coef(image_rows, text_rows, image_ids, text_ids, scale, shift)
    image_part = jnp.dot(coef, text_rows, preferred_element_type=f32)
    text_part = lax.dot_general(
        coef, image_rows, (((0,), (0,)), ((), ())), preferred_element_type=f32
    )

    part = [text_part[k * ex : (k + 1) * ex] for k in range(NY * NH)]
    part[4] = part[4] + hop(part[6].astype(bf16), up_y)
    part[3] = part[3] + hop(part[7].astype(bf16), down_y)
    own, oth = (
        part[k] + hop(part[k + 4].astype(bf16), up_y) + hop(part[k + 2].astype(bf16), down_y)
        for k in range(2)
    )
    own_send, oth_send = own.astype(bf16), oth.astype(bf16)
    text_grad = (
        own
        + hop(own_send, lambda m, z, y, h, c: None if m else (1, z, y, h, c))
        + hop(oth_send, lambda m, z, y, h, c: None if m else (1, z, y, 1 - h, c))
        + hop(oth_send, lambda m, z, y, h, c: (1, z, y, 1 - h, c) if m else None)
    )

    slab = [image_part[k * ex : (k + 1) * ex] for k in range(NZ)]
    end = slab[-1].astype(bf16)
    give = jnp.concatenate(
        [s.astype(bf16) for s in slab[2:7:2]] + [jnp.where(first, end[half:], end[:half])]
    )
    take = hop(give, swap)
    acc = jnp.where(first, slab[-1][:half], slab[-1][half:]) + take[-half:]
    came = hop(acc.astype(bf16), unring).astype(f32)
    pad = jnp.zeros_like(came)
    came = jnp.where(first, jnp.concatenate([came, pad]), jnp.concatenate([pad, came]))
    for k in (2, 1, 0):
        acc = slab[1 + 2 * k] + take[k * ex : (k + 1) * ex] + came
        came = hop(acc.astype(bf16), unring).astype(f32)
    mine = slab[0] + came
    mine_send = mine.astype(bf16)
    fa = hop(mine_send, lambda m, z, y, h, c: (0, z, y, h, m) if c else None)
    fb = hop(mine_send, lambda m, z, y, h, c: (0, z, y, h, 1) if m and not c else None)
    image_grad = jnp.where(first, mine, fb) + fa

    return jnp.where(image_side, image_grad, text_grad)[None]


def solution(mesh):
    placed = (P("tower", "blk", None), P("tower", None), P("tower", None, None), P(), P(), P())
    return jax.shard_map(
        on_device, mesh=mesh, in_specs=placed, out_specs=P("tower", "blk", None), check_vma=False
    )
```

```python
import jax
import jax.numpy as jnp
from jax import lax
from jax.sharding import PartitionSpec as P

NZ, NY, NH, NC = 8, 4, 2, 2
BLK = NZ * NY * NH * NC


def hop(value, route):
    pairs = []
    for m in range(2):
        for b in range(BLK):
            c, h, y, z = b % NC, b // NC % NH, b // (NC * NH) % NY, b // (NC * NH * NY)
            goal = route(m, z, y, h, c)
            if goal is None:
                continue
            tm, tz, ty, th, tc = goal
            target = ((tz % NZ * NY + ty % NY) * NH + th) * NC + tc
            pairs.append((m * BLK + b, tm * BLK + target))
    return lax.ppermute(value, ("tower", "blk"), pairs)


def to_spread(z, y, h, c, tower=0):
    return (tower, z, y, h if c else 1 - h, c)


def to_column(z, y, h, c, tower=0):
    return (tower, z, y, 1 - h if c else h, c)


def all_to_all_y(value):
    groups = [
        [m * BLK + ((z * NY + y) * NH + h) * NC + c for y in range(NY)]
        for m in range(2)
        for z in range(NZ)
        for h in range(NH)
        for c in range(NC)
    ]
    return lax.all_to_all(value, ("tower", "blk"), 0, 0, axis_index_groups=groups)


def embed_rows(feats, gain, weight):
    values = feats.astype(jnp.float32)
    center = values - jnp.mean(values, axis=-1, keepdims=True)
    spread = jnp.mean(center * center, axis=-1, keepdims=True)
    normed = (center * lax.rsqrt(spread + 1e-06) * gain).astype(jnp.bfloat16)
    head = jnp.dot(normed, weight, preferred_element_type=jnp.float32)
    length = jnp.sum(head * head, axis=-1, keepdims=True)
    return (head * lax.rsqrt(length + 1e-06)).astype(jnp.bfloat16)


def pair_coef(image_rows, text_rows, image_ids, text_ids, scale, shift):
    logits = (
        scale
        * lax.dot_general(
            image_rows, text_rows, (((1,), (1,)), ((), ())), preferred_element_type=jnp.float32
        )
        + shift
    )
    match = image_ids[:, None] == text_ids[None, :]
    share = jax.nn.sigmoid(jnp.where(match, -logits, logits))
    return jnp.where(match, -share, share).astype(jnp.bfloat16)


def on_device(pooled, final_gain, head_weight, pair_ids, log_scale, bias):
    bf16, f32 = jnp.bfloat16, jnp.float32
    local = embed_rows(pooled[0], final_gain[0], head_weight[0])
    ex, width = local.shape
    scale = jnp.exp(log_scale[0])
    shift = bias[0]
    m = lax.axis_index("tower")
    b = lax.axis_index("blk")
    c, h, y, z = b % NC, b // NC % NH, b // (NC * NH) % NY, b // (NC * NH * NY)
    keeper = c == m
    text_side = m == 1
    side = jnp.where(text_side | (c == 0), 1 - h, h)

    column = all_to_all_y(jnp.broadcast_to(local, (NY, ex, width)))
    near = hop(local, lambda m, z, y, h, c: to_spread(z, y, h, c) if m else ((1, z, y, h, 1) if c else None))
    across = hop(local, lambda m, z, y, h, c: (1, z, y, 1 - h, c) if m else None)
    prev = hop(local, lambda m, z, y, h, c: None if m else (c, z + 1, y, h, c))
    succ = hop(local, lambda m, z, y, h, c: None if m else (c, z - 1, y, h, c))
    opp = hop(local, lambda m, z, y, h, c: None if m else (c, z + 4, y, h, c))
    self_image = jnp.where(text_side, near, local)
    ring_a = jnp.concatenate([self_image, prev, succ, opp])

    spread = all_to_all_y(jnp.broadcast_to(jnp.where(text_side, across, near), (NY, ex, width)))
    other = hop(column.reshape(NY * ex, width), lambda m, z, y, h, c: to_column(z, y, h, c) if m else None)
    low = hop(jnp.concatenate([succ, opp]), lambda m, z, y, h, c: (m, z - 1, y, h, c) if m == c else None)
    high = hop(jnp.concatenate([prev, opp]), lambda m, z, y, h, c: (m, z + 1, y, h, c) if m == c else None)
    ring_b = jnp.concatenate([low, high])
    give = lambda m, z, y, h, c: (m, z, y, h, 1 - c) if m == c else None
    take = lambda m, z, y, h, c: None if m == c else (m, z, y, h, 1 - c)
    image_rows = jnp.concatenate(
        [jnp.where(keeper, ring_a, hop(ring_a, give)), jnp.where(keeper, ring_b, hop(ring_b, give))]
    )
    text_rows = jnp.concatenate(
        [spread.reshape(NY * ex, width), jnp.where(text_side, column.reshape(NY * ex, width), other)]
    )

    ids = pair_ids.reshape(NZ, NY, NH, NC, ex)
    image_col = lax.dynamic_slice(ids, (0, y, h, m, 0), (NZ, 1, 1, 1, ex)).reshape(NZ, ex)
    image_col = lax.dynamic_slice_in_dim(jnp.concatenate([image_col, image_col]), z, NZ)
    image_ids = image_col[jnp.array([0, 7, 1, 4, 2, 5, 6, 3])].reshape(NZ * ex)
    text_col = lax.dynamic_slice(ids, (z, 0, 0, c, 0), (1, NY, NH, 1, ex)).reshape(NY, NH, ex)
    text_col = jnp.where(side == 0, text_col, text_col[:, ::-1])
    text_ids = text_col.transpose(1, 0, 2).reshape(NY * NH * ex)

    coef = pair_coef(image_rows, text_rows, image_ids, text_ids, scale, shift)
    over_images = (((0,), (0,)), ((), ()))
    text_part = lax.dot_general(coef, image_rows, over_images, preferred_element_type=f32)
    part_b = jnp.dot(coef[4 * ex :], text_rows, preferred_element_type=f32)
    part_a = jnp.dot(coef[: 4 * ex], text_rows, preferred_element_type=f32)

    spread_part, column_part = text_part[: NY * ex], text_part[NY * ex :]
    spread_sum = jnp.sum(
        all_to_all_y(spread_part.astype(bf16).reshape(NY, ex, width)).astype(f32), axis=0
    )
    column_part = column_part + hop(
        column_part.astype(bf16), lambda m, z, y, h, c: None if m else to_column(z, y, h, c, 1)
    )
    text_grad = jnp.sum(
        all_to_all_y(column_part.astype(bf16).reshape(NY, ex, width)).astype(f32), axis=0
    )

    part_b = part_b + hop(part_b.astype(bf16), take)
    part_a = part_a + hop(part_a.astype(bf16), take)
    send_b = part_b.astype(bf16)
    low = hop(send_b[: 2 * ex], lambda m, z, y, h, c: (m, z + 1, y, h, c) if m == c else None)
    high = hop(send_b[2 * ex :], lambda m, z, y, h, c: (m, z - 1, y, h, c) if m == c else None)
    self_part = part_a[:ex]
    prev_send = (part_a[ex : 2 * ex] + high[:ex]).astype(bf16)
    succ_send = (part_a[2 * ex : 3 * ex] + low[:ex]).astype(bf16)
    opp_send = (part_a[3 * ex :] + low[ex:].astype(f32) + high[ex:].astype(f32)).astype(bf16)
    prev = hop(prev_send, lambda m, z, y, h, c: (0, z - 1, y, h, c) if m == c else None)
    succ = hop(succ_send, lambda m, z, y, h, c: (0, z + 1, y, h, c) if m == c else None)
    opp = hop(opp_send, lambda m, z, y, h, c: (0, z + 4, y, h, c) if m == c else None)

    near = hop(
        jnp.where(text_side, self_part, spread_sum).astype(bf16),
        lambda m, z, y, h, c: ((0, z, y, h, 1) if c else None) if m else to_spread(z, y, h, c, 1),
    )
    across = hop(spread_sum.astype(bf16), lambda m, z, y, h, c: (1, z, y, 1 - h, c) if m else None)
    text_grad = text_grad + near + across
    image_grad = (
        jnp.where(keeper, self_part, near.astype(f32)) + prev.astype(f32) + succ.astype(f32) + opp
    )
    return jnp.where(text_side, text_grad, image_grad)[None]


def solution(mesh):
    placed = (P("tower", "blk", None), P("tower", None), P("tower", None, None), P(), P(), P())
    return jax.shard_map(
        on_device, mesh=mesh, in_specs=placed, out_specs=P("tower", "blk", None), check_vma=False
    )
```

```python
import jax
import jax.numpy as jnp
from jax import lax
from jax.sharding import PartitionSpec as P

NZ, NY, NH, NC = 8, 4, 2, 2
BLK = NZ * NY * NH * NC


def hop(value, route):
    pairs = []
    for m in range(2):
        for b in range(BLK):
            c, h, y, z = b % NC, b // NC % NH, b // (NC * NH) % NY, b // (NC * NH * NY)
            goal = route(m, z, y, h, c)
            if goal is None:
                continue
            tm, tz, ty, th, tc = goal
            target = ((tz % NZ * NY + ty % NY) * NH + th) * NC + tc
            pairs.append((m * BLK + b, tm * BLK + target))
    return lax.ppermute(value, ("tower", "blk"), pairs)


def embed_rows(feats, gain, weight):
    values = feats.astype(jnp.float32)
    center = values - jnp.mean(values, axis=-1, keepdims=True)
    spread = jnp.mean(center * center, axis=-1, keepdims=True)
    normed = (center * lax.rsqrt(spread + 1e-06) * gain).astype(jnp.bfloat16)
    head = jnp.dot(normed, weight, preferred_element_type=jnp.float32)
    length = jnp.sum(head * head, axis=-1, keepdims=True)
    return (head * lax.rsqrt(length + 1e-06)).astype(jnp.bfloat16)


def pair_coef(image_rows, text_rows, image_ids, text_ids, scale, shift):
    logits = (
        scale
        * lax.dot_general(
            image_rows, text_rows, (((1,), (1,)), ((), ())), preferred_element_type=jnp.float32
        )
        + shift
    )
    match = image_ids[:, None] == text_ids[None, :]
    share = jax.nn.sigmoid(jnp.where(match, -logits, logits))
    return jnp.where(match, -share, share).astype(jnp.bfloat16)


def up_y(m, z, y, h, c):
    return (m, z, y + 1, h, c)


def down_y(m, z, y, h, c):
    return (m, z, y - 1, h, c)


def ring_z(m, z, y, h, c):
    return (m, z - 1 if c else z + 1, y, h, c)


def unring_z(m, z, y, h, c):
    return (m, z + 1 if c else z - 1, y, h, c)


def over_z(m, z, y, h, c):
    return (m, z + 4, y, h, c)


def swap(m, z, y, h, c):
    return (m, z, y, h, 1 - c)


def to_tower(m, z, y, h, c):
    return (1 - m, z, y, h, c)


def to_ring(m, z, y, h, c):
    return (0, z, y, 1 - h, c) if m else (1, z, y, h, 1 - c)


def from_ring(m, z, y, h, c):
    return (0, z, y, h, 1 - c) if m else (1, z, y, 1 - h, c)


def to_same(m, z, y, h, c):
    return (1, z, y, 1 - h, c) if m else (0, z, y, h, 1 - c)


def pick(table, order, size):
    wanted = order[:, None] == jnp.arange(size, dtype=jnp.int32)[None, :]
    return jnp.sum(jnp.where(wanted[:, :, None], table[None], 0), axis=1)


def on_device(pooled, final_gain, head_weight, pair_ids, log_scale, bias):
    bf16, f32 = jnp.bfloat16, jnp.float32
    local = embed_rows(pooled[0], final_gain[0], head_weight[0])
    ex = local.shape[0]
    half = ex // 2
    scale = jnp.exp(log_scale[0])
    shift = bias[0]
    m = lax.axis_index("tower")
    b = lax.axis_index("blk")
    c, h, y, z = b & 1, (b >> 1) & 1, (b >> 2) & 3, b >> 4
    first = c == 0
    image_side = m == 0

    def mine(value):
        return jnp.where(first, value[:half], value[half:])

    def whole(own, other):
        return jnp.where(
            first, jnp.concatenate([own, other]), jnp.concatenate([other, own])
        )

    p1 = hop(local, to_tower)
    p2 = hop(local, to_ring)
    p3 = hop(local, to_same)
    image = jnp.where(image_side, jnp.where(first, local, p3), jnp.where(first, p2, p1))
    texts = jnp.concatenate([jnp.where(image_side, p1, local), jnp.where(image_side, p2, p3)])

    r1 = hop(image, ring_z)
    q4 = hop(mine(image), over_z)
    below = hop(texts, up_y)
    above = hop(texts, down_y)
    got = hop(jnp.concatenate([r1, q4]), swap)
    s1 = got[:ex]
    q4 = whole(q4, got[ex:])
    r2 = hop(jnp.concatenate([r1, q4]), ring_z)
    far_own = hop(below[:ex], up_y)
    far_oth = hop(above[ex:], down_y)
    s2 = hop(r2, swap)

    image_rows = jnp.concatenate([image, r1, s1, q4, r2, s2])
    text_rows = jnp.concatenate([texts, below, above, far_own, far_oth])

    ids = pair_ids.reshape(NZ, NY, NH, NC, ex)
    image_col = lax.dynamic_slice(ids, (0, y, h, m, 0), (NZ, 1, 1, 1, ex)).reshape(NZ, ex)
    way = jnp.where(first, -1, 1)
    image_ids = pick(
        image_col, (z + way * jnp.array([0, 1, -1, 4, 2, -3, -2, 3], jnp.int32)) & 7, NZ
    ).reshape(NZ * ex)
    text_col = lax.dynamic_slice(ids, (z, 0, 0, c, 0), (1, NY, NH, 1, ex)).reshape(NY * NH, ex)
    text_ids = pick(
        text_col,
        ((y + jnp.array([0, 0, -1, -1, 1, 1, 2, 2], jnp.int32)) & 3) * 2
        + (h ^ jnp.array([0, 1, 0, 1, 0, 1, 0, 1], jnp.int32)),
        NY * NH,
    ).reshape(NY * NH * ex)

    coef = pair_coef(image_rows, text_rows, image_ids, text_ids, scale, shift)
    text_part = lax.dot_general(
        coef, image_rows, (((0,), (0,)), ((), ())), preferred_element_type=f32
    )
    image_part = jnp.dot(coef, text_rows, preferred_element_type=f32)

    far_own = hop(text_part[6 * ex : 7 * ex].astype(bf16), up_y)
    far_oth = hop(text_part[7 * ex :].astype(bf16), down_y)
    s2 = hop(image_part[6 * ex :].astype(bf16), swap)
    r2 = hop((image_part[4 * ex : 6 * ex] + s2).astype(bf16), unring_z)
    above = text_part[4 * ex : 6 * ex] + jnp.concatenate([far_own, jnp.zeros_like(far_own)])
    below = text_part[2 * ex : 4 * ex] + jnp.concatenate([jnp.zeros_like(far_oth), far_oth])
    above = hop(above.astype(bf16), up_y)
    below = hop(below.astype(bf16), down_y)
    q4 = image_part[3 * ex : 4 * ex] + r2[ex:]
    other_half = jnp.where(first, q4[half:], q4[:half])
    got = hop(
        jnp.concatenate([image_part[2 * ex : 3 * ex], other_half]).astype(bf16), swap
    )
    r1 = hop((image_part[ex : 2 * ex] + r2[:ex] + got[:ex]).astype(bf16), unring_z)
    q4 = hop((mine(q4) + got[ex:]).astype(bf16), over_z)
    image_sum = image_part[:ex] + r1 + whole(q4, jnp.zeros_like(q4))
    text_sum = text_part[: 2 * ex] + above + below

    image_send, text_send = image_sum.astype(bf16), text_sum.astype(bf16)
    p1 = hop(jnp.where(image_side, text_send[:ex], image_send), to_tower)
    p2 = hop(jnp.where(image_side, text_send[ex:], image_send), from_ring)
    p3 = hop(jnp.where(image_side, image_send, text_send[ex:]), to_same)
    p1, p2, p3 = p1.astype(f32), p2.astype(f32), p3.astype(f32)
    image_grad = jnp.where(first, image_sum + p3, p1 + p2)
    text_grad = text_sum[:ex] + p1 + p2 + p3
    return jnp.where(image_side, image_grad, text_grad)[None]


def solution(mesh):
    placed = (P("tower", "blk", None), P("tower", None), P("tower", None, None), P(), P(), P())
    return jax.shard_map(
        on_device, mesh=mesh, in_specs=placed, out_specs=P("tower", "blk", None), check_vma=False
    )
```

```python
import jax
import jax.numpy as jnp
from jax import lax
from jax.sharding import PartitionSpec as P


NZ, NY, NH, NC = 8, 4, 2, 2
BLK = NZ * NY * NH * NC


def hop(value, route):
    pairs = []
    for m in range(2):
        for b in range(BLK):
            c, h, y, z = b % NC, b // NC % NH, b // (NC * NH) % NY, b // (NC * NH * NY)
            goal = route(m, z, y, h, c)
            if goal is None:
                continue
            tm, tz, ty, th, tc = goal
            target = ((tz % NZ * NY + ty % NY) * NH + th) * NC + tc
            pairs.append((m * BLK + b, tm * BLK + target))
    return lax.ppermute(value, ("tower", "blk"), pairs)


def embed_rows(feats, gain, weight):
    values = feats.astype(jnp.float32)
    center = values - jnp.mean(values, axis=-1, keepdims=True)
    spread = jnp.mean(center * center, axis=-1, keepdims=True)
    normed = (center * lax.rsqrt(spread + 1e-06) * gain).astype(jnp.bfloat16)
    head = jnp.dot(normed, weight, preferred_element_type=jnp.float32)
    length = jnp.sum(head * head, axis=-1, keepdims=True)
    return (head * lax.rsqrt(length + 1e-06)).astype(jnp.bfloat16)


def pair_coef(image_rows, text_rows, image_ids, text_ids, scale, shift):
    logits = (
        scale
        * lax.dot_general(
            image_rows, text_rows, (((1,), (1,)), ((), ())), preferred_element_type=jnp.float32
        )
        + shift
    )
    match = image_ids[:, None] == text_ids[None, :]
    share = jax.nn.sigmoid(jnp.where(match, -logits, logits))
    return jnp.where(match, -share, share).astype(jnp.bfloat16)


def up_y(m, z, y, h, c):
    return (m, z, y + 1, h, c)


def down_y(m, z, y, h, c):
    return (m, z, y - 1, h, c)


def two_y(m, z, y, h, c):
    return (m, z, y + 2, h, c)


def ring_z(m, z, y, h, c):
    return (m, z - 1 if c else z + 1, y, h, c)


def unring_z(m, z, y, h, c):
    return (m, z + 1 if c else z - 1, y, h, c)


def ring2_z(m, z, y, h, c):
    return (m, z - 2 if c else z + 2, y, h, c)


def unring2_z(m, z, y, h, c):
    return (m, z + 2 if c else z - 2, y, h, c)


def swap(m, z, y, h, c):
    return (m, z, y, h, 1 - c)


def to_spread(m, z, y, h, c):
    if not m:
        return (1, z, y, h, 1) if c else None
    return (0, z, y, h if c else 1 - h, c)


def from_spread(m, z, y, h, c):
    if m:
        return (0, z, y, h, 1) if c else None
    return (1, z, y, h if c else 1 - h, c)


def forward(m, z, y, h, c):
    return None if m else (1, z, y, 1 - h if c else h, c)


def to_same(m, z, y, h, c):
    return (1, z, y, 1 - h, c) if m else None


def to_column(m, z, y, h, c):
    return (0, z, y, 1 - h if c else h, c) if m else None


def from_column(m, z, y, h, c):
    return None if m else (1, z, y, 1 - h if c else h, c)


def spread_y(block):
    below = hop(block, up_y)
    above = hop(block, down_y)
    far = hop(block, two_y)
    return jnp.concatenate([block, below, above, far])


def collect_y(part, ex):
    send = part[ex:].astype(jnp.bfloat16)
    below = hop(send[:ex], down_y)
    above = hop(send[ex : 2 * ex], up_y)
    far = hop(send[2 * ex :], two_y)
    return part[:ex] + below.astype(jnp.float32) + above.astype(jnp.float32) + far.astype(jnp.float32)


def pick(table, order, size):
    wanted = order[:, None] == jnp.arange(size, dtype=jnp.int32)[None, :]
    return jnp.sum(jnp.where(wanted[:, :, None], table[None], 0), axis=1)


def tile(pooled, final_gain, head_weight, pair_ids, log_scale, bias):
    bf16, f32 = jnp.bfloat16, jnp.float32
    local = embed_rows(pooled[0], final_gain[0], head_weight[0])
    ex = local.shape[0]
    half = ex // 2
    scale = jnp.exp(log_scale[0])
    shift = bias[0]
    m = lax.axis_index("tower")
    b = lax.axis_index("blk")
    c, h, y, z = b & 1, (b >> 1) & 1, (b >> 2) & 3, b >> 4
    first = c == 0
    image_side = m == 0
    side = jnp.where(image_side & (c == 1), h, 1 - h)

    def mine(value):
        return jnp.where(first, value[:half], value[half:])

    def whole(own, other):
        return jnp.where(
            first, jnp.concatenate([own, other]), jnp.concatenate([other, own])
        )

    near = hop(local, to_spread)
    column = spread_y(local)
    kept = jnp.where(image_side, local, near)
    image = jnp.where(c == m, kept, hop(kept, swap))
    across = hop(near, forward)
    near, image = lax.optimization_barrier((near, image))
    r1 = hop(image, ring_z)
    r2 = hop(image, ring2_z)
    spread = spread_y(jnp.where(image_side, near, across))
    other = hop(column, to_column)
    r3 = hop(r2, ring_z)
    r4 = hop(mine(r2), ring2_z)
    s12 = hop(jnp.concatenate([r1, r2]), swap)
    got = hop(jnp.concatenate([r3, r4]), swap)
    image_rows = jnp.concatenate([image, r1, r2, s12, r3, got[:ex], whole(r4, got[ex:])])
    text_rows = jnp.concatenate([spread, jnp.where(image_side, other, column)])

    ids = pair_ids.reshape(NZ, NY, NH, NC, ex)
    image_col = lax.dynamic_slice(ids, (0, y, h, m, 0), (NZ, 1, 1, 1, ex)).reshape(NZ, ex)
    way = jnp.where(first, -1, 1)
    image_ids = pick(
        image_col, (z + way * jnp.array([0, 1, 2, -1, -2, 3, -3, 4], jnp.int32)) & 7, NZ
    ).reshape(NZ * ex)
    text_col = lax.dynamic_slice(ids, (z, 0, 0, c, 0), (1, NY, NH, 1, ex)).reshape(NY * NH, ex)
    text_ids = pick(
        text_col,
        ((y + jnp.array([0, -1, 1, 2, 0, -1, 1, 2], jnp.int32)) & 3) * 2
        + (side ^ jnp.array([0, 0, 0, 0, 1, 1, 1, 1], jnp.int32)),
        NY * NH,
    ).reshape(NY * NH * ex)

    coef = pair_coef(image_rows, text_rows, image_ids, text_ids, scale, shift)
    text_part = lax.dot_general(
        coef, image_rows, (((0,), (0,)), ((), ())), preferred_element_type=f32
    )
    image_part = jnp.dot(coef, text_rows, preferred_element_type=f32)

    part = [image_part[k * ex : (k + 1) * ex] for k in range(NZ)]
    theirs = jnp.where(first, part[7][half:], part[7][:half])
    got = hop(jnp.concatenate([part[3], part[4], part[6], theirs]).astype(bf16), swap)
    r3 = hop((part[5] + got[2 * ex : 3 * ex]).astype(bf16), unring_z)
    r4 = hop((mine(part[7]) + got[3 * ex :]).astype(bf16), unring2_z)
    r1 = hop((part[1] + got[:ex]).astype(bf16), unring_z)
    r2 = part[2] + got[ex : 2 * ex].astype(f32) + r3.astype(f32) + whole(r4, jnp.zeros_like(r4))
    r2 = hop(r2.astype(bf16), unring2_z)
    image_sum = part[0] + r1.astype(f32) + r2.astype(f32)

    column_part = text_part[NY * ex :]
    column_part = column_part + hop(column_part.astype(bf16), from_column)
    spread_sum = collect_y(text_part[: NY * ex], ex)
    text_sum = collect_y(column_part, ex)
    spread_sum = lax.optimization_barrier(spread_sum.astype(bf16))
    across = hop(spread_sum, to_same)
    image_sum = image_sum + hop(image_sum.astype(bf16), swap)
    near = hop(jnp.where(image_side, spread_sum, image_sum.astype(bf16)), from_spread)
    near = near.astype(f32)
    image_grad = jnp.where(first, image_sum, near)
    text_grad = text_sum + near + across.astype(f32)
    return jnp.where(image_side, image_grad, text_grad)[None]


def solution(mesh):
    placed = (P("tower", "blk", None), P("tower", None), P("tower", None, None), P(), P(), P())
    return jax.shard_map(
        tile, mesh=mesh, in_specs=placed, out_specs=P("tower", "blk", None), check_vma=False
    )
```

```python
import jax
import jax.numpy as jnp
from jax import lax
from jax.experimental import pallas as pl
from jax.experimental.pallas import tpu as pltpu
from jax.sharding import PartitionSpec as P


NZ, NY, NH, NC = 8, 4, 2, 2
BLK = NZ * NY * NH * NC


def hop(value, route):
    pairs = []
    for m in range(2):
        for b in range(BLK):
            c, h, y, z = b % NC, b // NC % NH, b // (NC * NH) % NY, b // (NC * NH * NY)
            goal = route(m, z, y, h, c)
            if goal is None:
                continue
            tm, tz, ty, th, tc = goal
            target = ((tz % NZ * NY + ty % NY) * NH + th) * NC + tc
            pairs.append((m * BLK + b, tm * BLK + target))
    return lax.ppermute(value, ("tower", "blk"), pairs)


COLUMN_CUTS = 1


def embed_kernel(feats_hbm, gain_hbm, weight, out, feats, gain, staged, head, sems):
    cut = staged.shape[2]
    ahead = [
        pltpu.make_async_copy(feats_hbm.at[0], feats, sems.at[COLUMN_CUTS]),
        pltpu.make_async_copy(gain_hbm, gain, sems.at[COLUMN_CUTS + 1]),
    ]
    copies = [
        pltpu.make_async_copy(weight.at[0, :, pl.ds(k * cut, cut)], staged.at[k], sems.at[k])
        for k in range(COLUMN_CUTS)
    ]
    for copy in ahead + copies:
        copy.start()
    for copy in ahead:
        copy.wait()
    values = feats[...].astype(jnp.float32)
    center = values - jnp.mean(values, axis=-1, keepdims=True)
    spread = jnp.mean(center * center, axis=-1, keepdims=True)
    normed = (center * lax.rsqrt(spread + 1e-06) * gain[...]).astype(jnp.bfloat16)
    length = jnp.zeros((values.shape[0], 1), jnp.float32)
    for k, copy in enumerate(copies):
        copy.wait()
        part = jnp.dot(normed, staged[k], preferred_element_type=jnp.float32)
        length = length + jnp.sum(part * part, axis=-1, keepdims=True)
        head[k] = part
    factor = lax.rsqrt(length + 1e-06)
    for k in range(COLUMN_CUTS):
        out[:, k * cut : (k + 1) * cut] = (head[k] * factor).astype(jnp.bfloat16)


def embed_rows(feats, gain, weight):
    _, ex, width = feats.shape
    cut = width // COLUMN_CUTS
    return pl.pallas_call(
        embed_kernel,
        out_shape=jax.ShapeDtypeStruct((ex, width), jnp.bfloat16),
        in_specs=[pl.BlockSpec(memory_space=pltpu.HBM)] * 3,
        out_specs=pl.BlockSpec(memory_space=pltpu.VMEM),
        scratch_shapes=[
            pltpu.VMEM((ex, width), jnp.bfloat16),
            pltpu.VMEM((1, width), jnp.float32),
            pltpu.VMEM((COLUMN_CUTS, width, cut), jnp.bfloat16),
            pltpu.VMEM((COLUMN_CUTS, ex, cut), jnp.float32),
            pltpu.SemaphoreType.DMA((COLUMN_CUTS + 2,)),
        ],
        compiler_params=pltpu.CompilerParams(vmem_limit_bytes=66_400_000),
        name="embed",
    )(feats, gain, weight)


def pair_coef(image_rows, text_rows, image_ids, text_ids, scale, shift):
    logits = (
        scale
        * lax.dot_general(
            image_rows, text_rows, (((1,), (1,)), ((), ())), preferred_element_type=jnp.float32
        )
        + shift
    )
    match = image_ids[:, None] == text_ids[None, :]
    share = jax.nn.sigmoid(jnp.where(match, -logits, logits))
    return jnp.where(match, -share, share).astype(jnp.bfloat16)


def up_y(m, z, y, h, c):
    return (m, z, y + 1, h, c)


def down_y(m, z, y, h, c):
    return (m, z, y - 1, h, c)


def two_y(m, z, y, h, c):
    return (m, z, y + 2, h, c)


def ring_z(m, z, y, h, c):
    return (m, z - 1 if c else z + 1, y, h, c)


def unring_z(m, z, y, h, c):
    return (m, z + 1 if c else z - 1, y, h, c)


def ring2_z(m, z, y, h, c):
    return (m, z - 2 if c else z + 2, y, h, c)


def unring2_z(m, z, y, h, c):
    return (m, z + 2 if c else z - 2, y, h, c)


def swap(m, z, y, h, c):
    return (m, z, y, h, 1 - c)


def to_spread(m, z, y, h, c):
    if not m:
        return (1, z, y, h, 1) if c else None
    return (0, z, y, h if c else 1 - h, c)


def from_spread(m, z, y, h, c):
    if m:
        return (0, z, y, h, 1) if c else None
    return (1, z, y, h if c else 1 - h, c)


def forward(m, z, y, h, c):
    return None if m else (1, z, y, 1 - h if c else h, c)


def to_same(m, z, y, h, c):
    return (1, z, y, 1 - h, c) if m else None


def to_column(m, z, y, h, c):
    return (0, z, y, 1 - h if c else h, c) if m else None


def from_column(m, z, y, h, c):
    return None if m else (1, z, y, 1 - h if c else h, c)


def spread_y(block):
    below = hop(block, up_y)
    above = hop(block, down_y)
    far = hop(block, two_y)
    return jnp.concatenate([block, below, above, far])


def collect_y(part, ex):
    send = part[ex:].astype(jnp.bfloat16)
    below = hop(send[:ex], down_y)
    above = hop(send[ex : 2 * ex], up_y)
    far = hop(send[2 * ex :], two_y)
    return (
        part[:ex]
        + below.astype(jnp.float32)
        + above.astype(jnp.float32)
        + far.astype(jnp.float32)
    )


def pick(table, order, size):
    wanted = order[:, None] == jnp.arange(size, dtype=jnp.int32)[None, :]
    return jnp.sum(jnp.where(wanted[:, :, None], table[None], 0), axis=1)


def tile(pooled, final_gain, head_weight, pair_ids, log_scale, bias):
    bf16, f32 = jnp.bfloat16, jnp.float32
    local = embed_rows(pooled, final_gain, head_weight)
    ex = local.shape[0]
    half = ex // 2
    scale = jnp.exp(log_scale[0])
    shift = bias[0]
    m = lax.axis_index("tower")
    b = lax.axis_index("blk")
    c, h, y, z = b & 1, (b >> 1) & 1, (b >> 2) & 3, b >> 4
    first = c == 0
    image_side = m == 0
    side = jnp.where(image_side & (c == 1), h, 1 - h)

    def mine(value):
        return jnp.where(first, value[:half], value[half:])

    def whole(own, other):
        return jnp.where(
            first, jnp.concatenate([own, other]), jnp.concatenate([other, own])
        )

    near = hop(local, to_spread)
    column = spread_y(local)
    kept = jnp.where(image_side, local, near)
    image = jnp.where(c == m, kept, hop(kept, swap))
    across = hop(near, forward)
    near, image = lax.optimization_barrier((near, image))
    r1 = hop(image, ring_z)
    r2 = hop(image, ring2_z)
    spread = spread_y(jnp.where(image_side, near, across))
    other = hop(column, to_column)
    r3 = hop(r2, ring_z)
    r4 = hop(mine(r2), ring2_z)
    s12 = hop(jnp.concatenate([r1, r2]), swap)
    got = hop(jnp.concatenate([r3, r4]), swap)
    image_rows = jnp.concatenate([image, r1, r2, s12, r3, got[:ex], whole(r4, got[ex:])])
    text_rows = jnp.concatenate([spread, jnp.where(image_side, other, column)])

    ids = pair_ids.reshape(NZ, NY, NH, NC, ex)
    image_col = lax.dynamic_slice(ids, (0, y, h, m, 0), (NZ, 1, 1, 1, ex)).reshape(NZ, ex)
    way = jnp.where(first, -1, 1)
    image_ids = pick(
        image_col, (z + way * jnp.array([0, 1, 2, -1, -2, 3, -3, 4], jnp.int32)) & 7, NZ
    ).reshape(NZ * ex)
    text_col = lax.dynamic_slice(ids, (z, 0, 0, c, 0), (1, NY, NH, 1, ex)).reshape(NY * NH, ex)
    text_ids = pick(
        text_col,
        ((y + jnp.array([0, -1, 1, 2, 0, -1, 1, 2], jnp.int32)) & 3) * 2
        + (side ^ jnp.array([0, 0, 0, 0, 1, 1, 1, 1], jnp.int32)),
        NY * NH,
    ).reshape(NY * NH * ex)

    coef = pair_coef(image_rows, text_rows, image_ids, text_ids, scale, shift)
    text_part = lax.dot_general(
        coef, image_rows, (((0,), (0,)), ((), ())), preferred_element_type=f32
    )
    image_part = jnp.dot(coef, text_rows, preferred_element_type=f32)

    part = [image_part[k * ex : (k + 1) * ex] for k in range(NZ)]
    theirs = jnp.where(first, part[7][half:], part[7][:half])
    got = hop(jnp.concatenate([part[3], part[4], part[6], theirs]).astype(bf16), swap)
    r3 = hop((part[5] + got[2 * ex : 3 * ex]).astype(bf16), unring_z)
    r4 = hop((mine(part[7]) + got[3 * ex :]).astype(bf16), unring2_z)
    r1 = hop((part[1] + got[:ex]).astype(bf16), unring_z)
    r2 = part[2] + got[ex : 2 * ex].astype(f32) + r3.astype(f32) + whole(r4, jnp.zeros_like(r4))
    r2_send = r2.astype(bf16)
    r2 = hop(r2_send, unring2_z)
    image_sum = part[0] + r1.astype(f32) + r2.astype(f32)

    column_part = text_part[NY * ex :]
    came = hop(column_part.astype(bf16), from_column)
    column_part, _ = lax.optimization_barrier((column_part, r2_send))
    column_part = column_part + came
    spread_sum = collect_y(text_part[: NY * ex], ex)
    text_sum = collect_y(column_part, ex)
    spread_sum = lax.optimization_barrier(spread_sum.astype(bf16))
    across = hop(spread_sum, to_same)
    image_sum = image_sum + hop(image_sum.astype(bf16), swap)
    near = hop(jnp.where(image_side, spread_sum, image_sum.astype(bf16)), from_spread)
    near = near.astype(f32)
    image_grad = jnp.where(first, image_sum, near)
    text_grad = text_sum + near + across.astype(f32)
    return jnp.where(image_side, image_grad, text_grad)[None]


def solution(mesh):
    placed = (P("tower", "blk", None), P("tower", None), P("tower", None, None), P(), P(), P())
    return jax.shard_map(
        tile, mesh=mesh, in_specs=placed, out_specs=P("tower", "blk", None), check_vma=False
    )
```
